32 devices in a mesh: block: 4 (over y, x), span: 4 (over z), heads: 2 (over core).
Axes of the slice: x: 2, y: 2, z: 4, core: 2. Of those that a mesh axis runs over, the one named last changes fastest.
Arguments:
- fresh_keys: bfloat16 [16, 8192, 8, 128], P(None, ('block', 'span'), 'heads'), may hold values from -6 to 6
- fresh_values: bfloat16 [16, 8192, 8, 128], P(None, ('block', 'span'), 'heads'), may hold values from -6 to 6
- turn_angle: float32 [8192, 64], replicated, may hold values from -3.140625 to 3.140625
Outputs:
- stored_keys: bfloat16 [16, 8192, 8, 128], P(('block', 'span'), None, 'heads')
- stored_values: bfloat16 [16, 8192, 8, 128], P(('block', 'span'), None, 'heads')
- key_scale: float32 [16, 8, 128], P(('block', 'span'), 'heads')
The draws below stay inside these ranges and needn't reach their ends.
All inputs are finite; a program needn't handle non-finite values. Where the reference program divides by a largest or mean magnitude, that divisor is 1e-20 or more.
Results may differ from the reference program's by a relative error of at most 0.001.
Values may be sent and summed in bfloat16 or wider, within the bound.
A program may use at most 192 MiB of HBM per device.

```python
import jax
import jax.numpy as jnp

BATCH = 16
LENGTH = 8192
KV_HEADS = 8
HEAD_SIZE = 128
HALF_HEAD = 64


def steps_of(own_key, dims, split, low, top_value):
    loudness, own = 1.0, jax.random.fold_in(own_key, 6)
    for axis_at, blocks in split:
        draws = jnp.exp(jax.random.uniform(jax.random.fold_in(own, axis_at), (blocks,), jnp.float32, low / len(split), top_value / len(split)))
        loudness = loudness * jnp.repeat(draws, dims[axis_at] // blocks).reshape([-1 if axis == axis_at else 1 for axis in range(len(dims))])
    return loudness


def gaussian(rng, extent, scale, most, pieces=(), held_as=jnp.bfloat16):
    factor_of = steps_of(rng, extent, pieces, -0.22, 0.18) if pieces else 1.0
    result = jax.random.normal(rng, extent, jnp.float32) * scale * factor_of
    return jnp.minimum(jnp.maximum(result, -most), most).astype(held_as)


def setup_inputs(seed: int = 0) -> dict:
    splits = jax.random.split(jax.random.key(seed), 4)
    fresh_keys = gaussian(splits[0], (BATCH, LENGTH, KV_HEADS, HEAD_SIZE), 1.0, 6.0, ((1, 16), (2, 2)))
    fresh_values = gaussian(splits[1], (BATCH, LENGTH, KV_HEADS, HEAD_SIZE), 1.0, 6.0, ((1, 16), (2, 2)))
    turn_angle = jnp.clip(jax.random.uniform(splits[2], (LENGTH, HALF_HEAD), jnp.float32, -3.140625, 3.140625), -3.140625, 3.140625)
    return {"fresh_keys": fresh_keys, "fresh_values": fresh_values, "turn_angle": turn_angle}


def rotate_pairs(vectors, angle):
    half = vectors.shape[-1] // 2
    cosine, sine = jnp.cos(angle)[None, :, None, :], jnp.sin(angle)[None, :, None, :]
    first, second = vectors[..., :half], vectors[..., half:]
    return jnp.concatenate([first * cosine - second * sine, second * cosine + first * sine], axis=-1)


def keys_in_place(plain_keys, angle):
    wide_keys = plain_keys.astype(jnp.float32)
    return rotate_pairs(wide_keys, angle)


def reference(fresh_keys, fresh_values, turn_angle):
    turned_keys = keys_in_place(fresh_keys, turn_angle)
    key_scale = jnp.max(jnp.abs(turned_keys), axis=1)
    narrow_keys = (turned_keys / key_scale[:, None]).astype(jnp.bfloat16)
    stored_keys = narrow_keys
    stored_values = fresh_values
    return stored_keys, stored_values, key_scale
```

```python
import jax
import jax.numpy as jnp
from jax import lax
from jax.sharding import PartitionSpec as P


def rotate_pairs(vectors, angle):
    half = vectors.shape[-1] // 2
    cosine, sine = (jnp.cos(angle)[None, :, None, :], jnp.sin(angle)[None, :, None, :])
    first, second = (vectors[..., :half], vectors[..., half:])
    return jnp.concatenate(
        [first * cosine - second * sine, second * cosine + first * sine], axis=-1
    )


def solution(mesh):
    spans = mesh.shape["span"]
    n = mesh.shape["block"] * spans
    far = [d for d in range(1, n) if d % spans == spans // 2]
    near = [d for d in range(1, n) if d % spans != spans // 2]
    steps = []
    share = -(-len(near) // max(len(far), 1))
    for at, d in enumerate(far):
        steps += [d] + near[at * share : (at + 1) * share]

    def send(x):
        rows = x.shape[0] // n
        me = lax.axis_index(("block", "span"))
        got = []
        for d in steps:
            there = lax.rem(me + d, n)
            block = lax.dynamic_slice_in_dim(lax.optimization_barrier(x), there * rows, rows, 0)
            moved = lax.ppermute(block, ("block", "span"), [(i, (i + d) % n) for i in range(n)])
            got.append((lax.rem(me + n - d, n), moved))
        return got

    def join(x, got, fill):
        rows, piece = x.shape[0] // n, x.shape[1]
        me = lax.axis_index(("block", "span"))
        own = lax.dynamic_slice_in_dim(x, me * rows, rows, 0)
        out = jnp.full((rows, n * piece) + x.shape[2:], fill, x.dtype)
        out = lax.dynamic_update_slice_in_dim(out, own, me * piece, 1)
        for owner, block in got:
            out = lax.dynamic_update_slice_in_dim(out, block, owner * piece, 1)
        return out

    def local(fresh_keys, fresh_values, turn_angle):
        key_blocks = send(fresh_keys)
        value_blocks = send(fresh_values)
        moved_keys = join(fresh_keys, key_blocks, key_blocks[0][1][0, 0, 0, 0])
        turned_keys = rotate_pairs(moved_keys.astype(jnp.float32), turn_angle)
        key_scale = jnp.max(jnp.abs(turned_keys), axis=1)
        narrow_keys = (turned_keys / key_scale[:, None]).astype(jnp.bfloat16)
        stored_values = join(fresh_values, value_blocks, narrow_keys[0, 0, 0, 0])
        return (narrow_keys, stored_values, key_scale)

    return jax.shard_map(
        local,
        mesh=mesh,
        in_specs=(
            P(None, ("block", "span"), "heads", None),
            P(None, ("block", "span"), "heads", None),
            P(),
        ),
        out_specs=(
            P(("block", "span"), None, "heads", None),
            P(("block", "span"), None, "heads", None),
            P(("block", "span"), "heads", None),
        ),
        check_vma=False,
    )
```

```python
import math

import jax
import jax.numpy as jnp
from jax import lax
from jax.experimental import pallas as pl
from jax.experimental.pallas import tpu as pltpu
from jax.sharding import PartitionSpec as P


HBM = pl.BlockSpec(memory_space=pltpu.HBM)


def rotate_pairs(vectors, angle):
    half = vectors.shape[-1] // 2
    cosine, sine = (jnp.cos(angle)[None, :, None, :], jnp.sin(angle)[None, :, None, :])
    first, second = (vectors[..., :half], vectors[..., half:])
    return jnp.concatenate(
        [first * cosine - second * sine, second * cosine + first * sine], axis=-1
    )


def carry(pairs, held, arrived, left):
    into = [pltpu.make_async_copy(a, held.at[i], arrived.at[i]) for i, (a, b) in enumerate(pairs)]
    away = [pltpu.make_async_copy(held.at[i], b, left.at[i]) for i, (a, b) in enumerate(pairs)]
    for copy in into:
        copy.start()
    for one, two in zip(into, away):
        one.wait()
        two.start()
    for copy in away:
        copy.wait()


def solution(mesh):
    axes = ("block", "span")
    n = mesh.shape["block"] * mesh.shape["span"]
    stride = next(k for k in range(min(7, n - 1), 0, -1) if math.gcd(k, n) == 1)
    steps = sorted(range(1, n), key=lambda d: (d * stride) % n)

    def peer(index, step, sign=1):
        return (index + n + sign * step) % n

    def params(count, x):
        rows = x.shape[0] // n
        size = count * rows * x.shape[1] * x.shape[2] * x.shape[3] * x.dtype.itemsize
        return dict(
            scratch_shapes=[
                pltpu.VMEM((count, rows) + x.shape[1:], x.dtype),
                pltpu.SemaphoreType.DMA((count,)),
                pltpu.SemaphoreType.DMA((count,)),
            ],
            compiler_params=pltpu.CompilerParams(vmem_limit_bytes=2 * size + 2**22),
            cost_estimate=pl.CostEstimate(flops=0, bytes_accessed=2 * size, transcendentals=0),
        )

    def cut(x, shifts, after):
        rows = x.shape[0] // n

        def kernel(x_ref, after_ref, *rest):
            outs, scratch = rest[: len(shifts)], rest[len(shifts) :]
            me = lax.axis_index(axes)
            carry(
                [(x_ref.at[pl.ds(peer(me, d) * rows, rows)], o) for d, o in zip(shifts, outs)],
                *scratch,
            )

        shape = jax.ShapeDtypeStruct((rows,) + x.shape[1:], x.dtype)
        return pl.pallas_call(
            kernel,
            out_shape=[shape] * len(shifts),
            in_specs=[HBM, HBM],
            out_specs=[HBM] * len(shifts),
            name="cut",
            **params(len(shifts), x),
        )(x, after)

    def shift(block, d):
        return lax.ppermute(block, axes, [(i, peer(i, d)) for i in range(n)])

    def join(x, shifts, blocks, whole, after):
        rows, piece = x.shape[0] // n, x.shape[1]

        def kernel(*refs):
            ins, out, scratch = refs[: len(shifts)], refs[-4], refs[-3:]
            me = lax.axis_index(axes)
            pairs = []
            for d, ref in zip(shifts, ins):
                at = peer(me, d, -1)
                source = ref if d else ref.at[pl.ds(me * rows, rows)]
                pairs.append((source, out.at[:, pl.ds(at * piece, piece)]))
            carry(pairs, *scratch)

        given = list(blocks) + [after] + ([] if whole is None else [whole])
        return pl.pallas_call(
            kernel,
            out_shape=jax.ShapeDtypeStruct((rows, n * piece) + x.shape[2:], x.dtype),
            in_specs=[HBM] * len(given),
            out_specs=HBM,
            input_output_aliases={} if whole is None else {len(given) - 1: 0},
            name="join",
            **params(len(shifts), x),
        )(*given)

    def whole(fresh_keys, fresh_values, turn_angle):
        rows = fresh_keys.shape[0] // n
        me = lax.axis_index(axes)
        lead = steps[0]
        first = lax.dynamic_slice_in_dim(fresh_keys, peer(me, lead) * rows, rows, 0)
        others = cut(fresh_keys, steps[1:], first)
        keys = [shift(b, d) for d, b in zip(steps, [first] + list(others))]
        cuts = cut(fresh_values, steps, others[0])
        values = [shift(b, d) for d, b in zip(steps, cuts)]
        moved_keys = join(fresh_keys, [0] + steps, [fresh_keys] + keys, None, first)
        turned_keys = rotate_pairs(moved_keys.astype(jnp.float32), turn_angle)
        key_scale = jnp.max(jnp.abs(turned_keys), axis=1)
        narrow_keys = (turned_keys / key_scale[:, None]).astype(jnp.bfloat16)
        ends = [n // 2, n - 4, n - 1]
        stored = join(fresh_values, [0] + steps[: ends[0]], [fresh_values] + values[: ends[0]], None, narrow_keys)
        for low, high in zip(ends, ends[1:]):
            stored = join(fresh_values, steps[low:high], values[low:high], stored, narrow_keys)
        return (narrow_keys, stored, key_scale)

    return jax.shard_map(
        whole,
        mesh=mesh,
        in_specs=(
            P(None, ("block", "span"), "heads", None),
            P(None, ("block", "span"), "heads", None),
            P(),
        ),
        out_specs=(
            P(("block", "span"), None, "heads", None),
            P(("block", "span"), None, "heads", None),
            P(("block", "span"), "heads", None),
        ),
        check_vma=False,
    )
```
